128 devices in a mesh: shard: 8 (over x, core), replica: 16 (over z, y).
Axes of the slice: x: 4, y: 4, z: 4, core: 2. Of those that a mesh axis runs over, the one named last changes fastest.
Arguments:
- gradients: bfloat16 [16, 128, 512, 512], P('replica', 'shard'), may hold values from -3 to 3
- first_moment: float32 [128, 512, 512], P(('shard', 'replica')), may hold values from -6 to 6
- second_moment: float32 [128, 512, 512], P(('shard', 'replica')), may hold values from 0.25 to 4
- left_stat: float32 [128, 512, 512], P(('shard', 'replica')), as said below
- right_stat: float32 [128, 512, 512], P(('shard', 'replica')), as said below
- left_basis: float32 [128, 512, 512], P(('shard', 'replica')), as said below
- right_basis: float32 [128, 512, 512], P(('shard', 'replica')), as said below
- refresh_flags: int32 [128], replicated, may hold values from 0 to 1, as said below
Outputs:
- direction: bfloat16 [128, 512, 512], P('shard')
- new_first: float32 [128, 512, 512], P(('shard', 'replica'))
- new_second: float32 [128, 512, 512], P(('shard', 'replica'))
- new_left: float32 [128, 512, 512], P(('shard', 'replica'))
- new_right: float32 [128, 512, 512], P(('shard', 'replica'))
- new_left_basis: float32 [128, 512, 512], P(('shard', 'replica'))
- new_right_basis: float32 [128, 512, 512], P(('shard', 'replica'))
The draws below stay inside these ranges and needn't reach their ends.
Inputs may be any that keep to these rules, and one draw needn't show every extreme that they name: Write b = ((p * 16 + q)) + j. For every q, j and k, exactly one of the two blocks with p = 2 k and p = 2 k + 1 has refresh_flags[b] = 1. `left_stat`: every block is symmetric positive definite with all eigenvalues 1 or more. `right_stat`: every block is symmetric positive definite with all eigenvalues 1 or more. `left_basis`: every block is an orthogonal matrix. `right_basis`: every block is an orthogonal matrix.
All inputs are finite; a program needn't handle non-finite values.
Results may differ from the reference program's by a relative error of at most 0.012.
Values may be sent and summed in bfloat16 or wider, within the bound.
No kernel may reach another device: no remote copies, remote signals or barrier semaphores. Data moves between devices by JAX's collectives and lax.ppermute only.
A program may use at most 128 MiB of HBM per device.

```python
import math
import jax
import jax.numpy as jnp
from jax import lax

BLOCK = 512
BLK_DEV = 1
POWER = 2
NBLK = 128
N_SHARD = 8
N_REPLICA = 16


def definite_blocks(key):
    key_diag, key_factor = jax.random.split(key)
    diagonal = jnp.exp(jax.random.uniform(key_diag, (NBLK, BLOCK), jnp.float32, 0.0, jnp.log(10.0)))
    factor = jax.random.normal(key_factor, (NBLK, BLOCK, BLOCK), jnp.float32)
    square = jnp.einsum('kij,klj->kil', factor, factor, precision=lax.Precision.HIGHEST) * (0.5 / BLOCK)
    square = 0.5 * (square + jnp.swapaxes(square, 1, 2))
    return square + jnp.eye(BLOCK, dtype=jnp.float32)[None, :, :] * diagonal[:, :, None]


def orthogonal_blocks(key):
    matrix = jax.random.normal(key, (NBLK, BLOCK, BLOCK), jnp.float32)
    basis, upper = jnp.linalg.qr(matrix)
    return basis


def draw_left_stat(key, part):
    return definite_blocks(jax.random.fold_in(key, 101))


def draw_right_stat(key, part):
    return definite_blocks(jax.random.fold_in(key, 102))


def draw_left_basis(key, part):
    return orthogonal_blocks(jax.random.fold_in(key, 103))


def draw_right_basis(key, part):
    return orthogonal_blocks(jax.random.fold_in(key, 104))


def draw_refresh_flags(key, part):
    picks = jax.random.randint(jax.random.fold_in(key, 105), (N_SHARD // 2, N_REPLICA, BLK_DEV), 0, 2)
    shard_ids = jnp.arange(N_SHARD, dtype=jnp.int32)
    chosen = picks[shard_ids // 2]
    flagged = (chosen == (shard_ids % 2)[:, None, None]).astype(jnp.int32)
    return flagged.reshape(NBLK)


def block_scale(own_key, dims, cuts, least, high):
    level = 1.0
    for dim, blocks in cuts:
        draws = jax.random.uniform(jax.random.fold_in(jax.random.fold_in(own_key, 6), dim), (blocks,), jnp.float32, least / len(cuts), high / len(cuts))
        level = level * jnp.repeat(jnp.exp(draws), dims[dim] // blocks).reshape((-1,) + (1,) * (len(dims) - 1 - dim))
    return level


def scatter_about(stream_key, shape, width, limit, cuts=(), kind=jnp.bfloat16):
    values = width * jax.random.normal(stream_key, shape, jnp.float32)
    if cuts:
        values = values * block_scale(stream_key, shape, cuts, -0.22, 0.18)
    return jnp.clip(values, -limit, limit).astype(kind)


def setup_inputs(seed: int = 0) -> dict:
    seeds = jax.random.split(jax.random.key(seed), 9)
    gradients = scatter_about(seeds[0], (N_REPLICA, NBLK, BLOCK, BLOCK), 0.5, 3.0, ((0, 16), (1, 8)))
    first_moment = scatter_about(seeds[1], (NBLK, BLOCK, BLOCK), 1.0, 6.0, ((0, 128),), jnp.float32)
    second_moment = jnp.clip(jnp.exp(math.log(4.0) - 2.7725887 * jax.random.uniform(seeds[2], (NBLK, BLOCK, BLOCK), jnp.float32) ** block_scale(seeds[2], (NBLK, BLOCK, BLOCK), ((0, 128),), -0.2, 0.2)), 0.25, 4.0)
    left_stat = draw_left_stat(jax.random.fold_in(seeds[8], 71), 0)
    right_stat = draw_right_stat(jax.random.fold_in(seeds[8], 71), 0)
    left_basis = draw_left_basis(jax.random.fold_in(seeds[8], 71), 0)
    right_basis = draw_right_basis(jax.random.fold_in(seeds[8], 71), 0)
    refresh_flags = draw_refresh_flags(jax.random.fold_in(seeds[8], 71), 0)
    return dict(gradients=gradients, first_moment=first_moment, second_moment=second_moment, left_stat=left_stat, right_stat=right_stat, left_basis=left_basis, right_basis=right_basis, refresh_flags=refresh_flags)


beta_one = 0.95
beta_two = 0.95
epsilon = 1e-08
bias_step = 10.0

def highest(left_side, right_side):
    return jnp.dot(left_side.astype(jnp.float32), right_side.astype(jnp.float32), precision=lax.Precision.HIGHEST, preferred_element_type=jnp.float32)

def orthonormal(matrix):
    gram = highest(matrix.T, matrix)
    lower_factor = jnp.linalg.cholesky(gram)
    return jax.scipy.linalg.solve_triangular(lower_factor, matrix.T, lower=True).T

def power_step(factor, basis):
    for repeat in range(POWER):
        product = jnp.dot(factor.astype(jnp.bfloat16).astype(jnp.float32), basis.astype(jnp.bfloat16).astype(jnp.float32), preferred_element_type=jnp.float32)
        basis = orthonormal(product)
    return basis

def update_block(grad_stack, moment, second, left_factor, right_factor, basis_old_left, basis_old_right, flagged):
    summed = lax.optimization_barrier(jnp.sum(grad_stack.astype(jnp.float32), axis=0))
    low_grad = summed.astype(jnp.bfloat16)
    left_new = beta_two * left_factor + (1.0 - beta_two) / BLOCK * jnp.dot(low_grad.astype(jnp.float32), low_grad.T.astype(jnp.float32), preferred_element_type=jnp.float32)
    right_new = beta_two * right_factor + (1.0 - beta_two) / BLOCK * jnp.dot(low_grad.T.astype(jnp.float32), low_grad.astype(jnp.float32), preferred_element_type=jnp.float32)

    def refresh_both():
        basis_left = power_step(left_new, basis_old_left)
        basis_right = power_step(right_new, basis_old_right)
        carried = highest(highest(highest(basis_left.T, basis_old_left), moment), highest(basis_old_right.T, basis_right))
        return (basis_left, basis_right, carried)

    def retain():
        return (basis_old_left, basis_old_right, moment)
    basis_left, basis_right, carried = lax.cond(flagged == 1, refresh_both, retain)
    rotated = highest(highest(basis_left.T, summed), basis_right)
    moment_new = beta_one * carried + (1.0 - beta_one) * rotated
    second_new = beta_two * second + (1.0 - beta_two) * rotated * rotated
    scaled = moment_new / (1.0 - beta_one ** bias_step) / (jnp.sqrt(second_new / (1.0 - beta_two ** bias_step)) + epsilon)
    direction = highest(highest(basis_left, scaled), basis_right.T).astype(jnp.bfloat16)
    return (direction, moment_new, second_new, left_new, right_new, basis_left, basis_right)

def reference(gradients, first_moment, second_moment, left_stat, right_stat, left_basis, right_basis, refresh_flags):

    def handle(position):
        pieces = [lax.dynamic_index_in_dim(array, position, 0, keepdims=False) for array in (first_moment, second_moment, left_stat, right_stat, left_basis, right_basis)]
        grad_stack = lax.dynamic_index_in_dim(gradients, position, 1, keepdims=False)
        flagged = lax.dynamic_index_in_dim(refresh_flags, position, 0, keepdims=False)
        return update_block(grad_stack, pieces[0], pieces[1], pieces[2], pieces[3], pieces[4], pieces[5], flagged)
    results = lax.map(handle, jnp.arange(NBLK, dtype=jnp.int32))
    return (results[0], results[1], results[2], results[3], results[4], results[5], results[6])
```

```python
import jax
import jax.numpy as jnp
from jax import lax
from jax.experimental import pallas as pl
from jax.experimental.pallas import tpu as pltpu
from jax.sharding import PartitionSpec as P

POWER = 2
PANEL = 128
GROUP = 8

beta_one = 0.95
beta_two = 0.95
epsilon = 1e-08
bias_step = 10.0

HIGHEST = lax.Precision.HIGHEST
NN = (((1,), (0,)), ((), ()))
NT = (((1,), (1,)), ((), ()))
TN = (((0,), (0,)), ((), ()))


def mm(left_side, right_side, dims, precision=HIGHEST):
    return lax.dot_general(
        left_side, right_side, dims, precision=precision, preferred_element_type=jnp.float32
    )


def low(left_side, right_side, dims):
    return lax.dot_general(
        left_side.astype(jnp.bfloat16),
        right_side.astype(jnp.bfloat16),
        dims,
        preferred_element_type=jnp.float32,
    )


def swapped(block, axis, stride):
    count = lax.axis_size(axis)
    route = []
    for low_id in range(count):
        high = low_id | 1 << stride
        if high != low_id and high < count:
            route += [(low_id, high), (high, low_id)]
    return lax.ppermute(block, axis, route)


def inverse_factor(rows, out_ref):
    shape = (GROUP, PANEL)
    lane = lax.broadcasted_iota(jnp.int32, shape, 1)
    count = PANEL // GROUP
    for group in range(count):
        start = group * GROUP
        pivot = rows[group]
        lines = [jnp.broadcast_to(pivot[q : q + 1, :], shape) for q in range(GROUP)]
        entry = [
            [
                jnp.broadcast_to(lines[q][:, start + p : start + p + 1], shape) if p >= q else None
                for p in range(GROUP)
            ]
            for q in range(GROUP)
        ]
        inside = (lane >= start) & (lane < start + GROUP)
        lines = [
            jnp.where(inside, jnp.where(lane == start + q, 1.0, 0.0), lines[q])
            for q in range(GROUP)
        ]
        inverse = []
        factor = [[None] * GROUP for _ in range(GROUP)]
        for q in range(GROUP):
            inverse.append(1.0 / entry[q][q])
            for p in range(q + 1, GROUP):
                factor[p][q] = entry[q][p] * inverse[q]
                for r in range(p, GROUP):
                    entry[p][r] = entry[p][r] - factor[p][q] * entry[q][r]
                lines[p] = lines[p] - factor[p][q] * lines[q]
            final = jnp.where(lane < start + GROUP, lines[q] * lax.rsqrt(entry[q][q]), 0.0)
            out_ref[start + q : start + q + 1, :] = final[0:1, :]
        if group + 1 == count:
            break
        solved = [None] * GROUP
        for q in reversed(range(GROUP)):
            value = lines[q] * inverse[q]
            for p in range(q + 1, GROUP):
                value = value - factor[p][q] * solved[p]
            solved[q] = value
        for i in range(group + 1, count):
            below = jnp.where(inside, 0.0, rows[i])
            for q in range(GROUP):
                column = jnp.broadcast_to(rows[i][:, start + q : start + q + 1], shape)
                below = below - column * solved[q]
            rows[i] = below


def refresh_kernel(factor_ref, basis_ref, out_ref, low_ref, gram_ref, prod_ref, inv_ref):
    side = out_ref.shape[0]
    low_ref[...] = basis_ref[...]

    def power(step, carry):
        prod_ref[...] = mm(factor_ref[...], low_ref[...], NN, None)
        gram_ref[...] = mm(prod_ref[...], prod_ref[...], TN)
        for start in range(0, side, PANEL):
            stop = start + PANEL
            rows = [
                gram_ref[i : i + GROUP, start:stop] for i in range(start, stop, GROUP)
            ]
            inverse_factor(rows, inv_ref)
            inv = inv_ref[...]
            ortho = mm(prod_ref[:, start:stop], inv, NT)
            out_ref[:, start:stop] = ortho
            if stop < side:
                upper = mm(inv, gram_ref[start:stop, stop:], NN)
                gram_ref[stop:, stop:] = gram_ref[stop:, stop:] - mm(upper, upper, TN)
                prod_ref[:, stop:] = prod_ref[:, stop:] - mm(ortho, upper, NN)
        low_ref[...] = out_ref[...].astype(jnp.bfloat16)
        return carry

    lax.fori_loop(0, POWER, power, 0)


def refresh(factor, basis):
    side = factor.shape[0]
    return pl.pallas_call(
        refresh_kernel,
        out_shape=(
            jax.ShapeDtypeStruct((side, side), jnp.float32),
            jax.ShapeDtypeStruct((side, side), jnp.bfloat16),
        ),
        in_specs=[pl.BlockSpec(memory_space=pltpu.VMEM)] * 2,
        out_specs=(pl.BlockSpec(memory_space=pltpu.VMEM),) * 2,
        scratch_shapes=[
            pltpu.VMEM((side, side), jnp.float32),
            pltpu.VMEM((side, side), jnp.float32),
            pltpu.VMEM((PANEL, PANEL), jnp.float32),
        ],
        name="refresh",
    )(factor, basis)


def update_kernel(
    flag_ref,
    new_left_ref,
    new_right_ref,
    old_left_ref,
    old_right_ref,
    summed_ref,
    spread_ref,
    first_ref,
    second_ref,
    direction_ref,
    first_out_ref,
    second_out_ref,
    left_out_ref,
    right_out_ref,
):
    renewed = flag_ref[0] == 1
    left = jnp.where(renewed, new_left_ref[...], old_left_ref[...])
    left_out_ref[...] = left
    left = left.astype(jnp.bfloat16)
    right = jnp.where(renewed, new_right_ref[...].astype(jnp.float32), old_right_ref[...])
    right_out_ref[...] = right
    right = right.astype(jnp.bfloat16)
    rotated = low(low(left, summed_ref[...], TN), right, NN)
    carried = low(low(left, spread_ref[...], TN), right, NN)
    carried = jnp.where(renewed, carried, first_ref[...])
    moment_new = beta_one * carried + (1.0 - beta_one) * rotated
    second_new = beta_two * second_ref[...] + (1.0 - beta_two) * rotated * rotated
    first_out_ref[...] = moment_new
    second_out_ref[...] = second_new
    scaled = (
        moment_new
        / (1.0 - beta_one**bias_step)
        / (jnp.sqrt(second_new / (1.0 - beta_two**bias_step)) + epsilon)
    )
    direction_ref[...] = low(low(left, scaled, NN), right, NT).astype(jnp.bfloat16)


def update(flag, *arrays):
    side = arrays[0].shape[0]
    block = jax.ShapeDtypeStruct((side, side), jnp.float32)
    vmem = pl.BlockSpec(memory_space=pltpu.VMEM)
    return pl.pallas_call(
        update_kernel,
        out_shape=(jax.ShapeDtypeStruct((side, side), jnp.bfloat16), block, block, block, block),
        in_specs=[pl.BlockSpec(memory_space=pltpu.SMEM)] + [vmem] * len(arrays),
        out_specs=(vmem,) * 5,
        name="update",
    )(flag, *arrays)


def local(
    gradients,
    first_moment,
    second_moment,
    left_stat,
    right_stat,
    left_basis,
    right_basis,
    refresh_flags,
):
    replica_count = lax.axis_size("replica")
    owner_id = lax.axis_index("shard") * replica_count + lax.axis_index("replica")
    flag = lax.dynamic_slice_in_dim(refresh_flags, owner_id, 1)
    renewed = flag[0] == 1
    old_left, old_right, first = left_basis[0], right_basis[0], first_moment[0]
    arrived_basis = swapped(old_right.astype(jnp.bfloat16), "shard", 0)
    start_basis = jnp.where(renewed, old_left.astype(jnp.bfloat16), arrived_basis)
    spread = mm(mm(old_left, first, NN), old_right, NT).astype(jnp.bfloat16)

    summed = lax.psum_scatter(gradients, "replica", scatter_dimension=1, tiled=True)[0, 0]
    summed, spread, start_basis = lax.optimization_barrier((summed, spread, start_basis))
    side = summed.shape[0]
    weight = (1.0 - beta_two) / side
    right_new = beta_two * right_stat[0] + weight * mm(summed, summed, TN, None)
    left_new = beta_two * left_stat[0] + weight * mm(summed, summed, NT, None)
    arrived_factor = swapped(right_new.astype(jnp.bfloat16), "shard", 0)
    factor = jnp.where(renewed, left_new.astype(jnp.bfloat16), arrived_factor)
    fresh, fresh_low = refresh(factor, start_basis)
    helped = swapped(fresh_low, "shard", 0)
    direction, first_new, second_new, basis_left, basis_right = update(
        flag, fresh, helped, old_left, old_right, summed, spread, first, second_moment[0]
    )
    gathered = lax.all_gather(direction[None], "replica", axis=0, tiled=True)
    return (
        gathered,
        first_new[None],
        second_new[None],
        left_new[None],
        right_new[None],
        basis_left[None],
        basis_right[None],
    )


def solution(mesh):
    owned = P(("shard", "replica"), None, None)
    in_specs = (P("replica", "shard", None, None),) + (owned,) * 6 + (P(),)
    out_specs = (P("shard", None, None),) + (owned,) * 6
    return jax.shard_map(local, mesh=mesh, in_specs=in_specs, out_specs=out_specs, check_vma=False)
```
